32 devices in a mesh: gx: 2 (over x), gy: 4 (over z), gz: 4 (over y, core).
Axes of the slice: x: 2, y: 2, z: 4, core: 2. Of those that a mesh axis runs over, the one named last changes fastest.
Arguments:
- pair_map: bfloat16 [160, 160, 128], P('gx', ('gy', 'gz')), may hold values from -6 to 6
- residue_mask: int32 [160], replicated, may hold values 0 or 1
- proj_weight: bfloat16 [128, 512], replicated, may hold values from -0.5 to 0.5
- gate_weight: bfloat16 [128, 128], replicated, may hold values from -0.5 to 0.5
- out_weight: bfloat16 [128, 128], replicated, may hold values from -0.5 to 0.5
Outputs:
- update: bfloat16 [160, 160, 128], P('gx', ('gy', 'gz'))
The draws below stay inside these ranges and needn't reach their ends.
All inputs are finite; a program needn't handle non-finite values.
Results may differ from the reference program's by a relative error of at most 0.009.
Values may be sent and summed in bfloat16 or wider, within the bound.
A program may use at most 128 MiB of HBM per device.

```python
import jax
import jax.numpy as jnp
from jax import lax

C = 128
HID = 128
RES_DEV = 80
N = 160


def touch_ends(result, key, least, top_value):
    dims = result.shape
    place = [jax.random.randint(jax.random.fold_in(key, axis), (), 0, dims[axis]) for axis in range(len(dims))]
    result = result.at[tuple(place)].set(least)
    longest = dims.index(max(dims))
    place[longest] = (place[longest] + 1) % dims[longest]
    return result.at[tuple(place)].set(top_value)


def steps_of(own_key, dims, pieces, smallest, high):
    gain, own = 1.0, jax.random.fold_in(own_key, 6)
    for axis_at, parts in pieces:
        heights = jnp.exp(jax.random.uniform(jax.random.fold_in(own, axis_at), (parts,), jnp.float32, smallest / len(pieces), high / len(pieces)))
        gain = gain * jnp.repeat(heights, dims[axis_at] // parts).reshape([-1 if axis == axis_at else 1 for axis in range(len(dims))])
    return gain


def gaussian(own_key, extent, deviation, bound, pieces=(), kind=jnp.bfloat16):
    entries = deviation * jax.random.normal(own_key, extent, jnp.float32)
    if pieces:
        entries = entries * steps_of(own_key, extent, pieces, -0.22, 0.18)
    return jnp.clip(entries, -bound, bound).astype(kind)


def setup_inputs(seed: int = 0) -> dict:
    splits = jax.random.split(jax.random.key(seed), 6)
    pair_map = gaussian(splits[0], (N, N, C), 1.0, 6.0, ((0, 2), (1, 16)))
    residue_mask = touch_ends((jax.random.randint(splits[1], (N,), 0, 8) < 7).astype(jnp.int32), jax.random.fold_in(splits[1], 1), 0, 1)
    proj_weight = gaussian(splits[2], (C, 4 * HID), C ** -0.5, 0.5)
    gate_weight = gaussian(splits[3], (C, C), C ** -0.5, 0.5)
    out_weight = gaussian(splits[4], (HID, C), HID ** -0.5, 0.5)
    return {"pair_map": pair_map, "residue_mask": residue_mask, "proj_weight": proj_weight, "gate_weight": gate_weight, "out_weight": out_weight}


epsilon = 1.0

def layer_norm(values):
    average = lax.optimization_barrier(jnp.mean(values, axis=-1, keepdims=True))
    centred = values - average
    variance = lax.optimization_barrier(jnp.mean(centred * centred, axis=-1, keepdims=True))
    return centred * lax.rsqrt(variance + epsilon)

def reference(pair_map, residue_mask, proj_weight, gate_weight, out_weight):
    mask_float = residue_mask.astype(jnp.float32)

    def project(inputs):
        row_block, row_mask = inputs
        normed = layer_norm(row_block.astype(jnp.float32)).astype(jnp.bfloat16)
        flattened = normed.reshape(-1, C)
        projected = jnp.dot(flattened, proj_weight, preferred_element_type=jnp.float32).reshape(RES_DEV, N, 4 * HID)
        pair_mask = (row_mask[:, None] * mask_float[None, :])[:, :, None]
        left_proj = (jax.nn.sigmoid(projected[:, :, :HID]) * projected[:, :, HID:2 * HID] * pair_mask).astype(jnp.bfloat16)
        right_proj = (jax.nn.sigmoid(projected[:, :, 2 * HID:3 * HID]) * projected[:, :, 3 * HID:] * pair_mask).astype(jnp.bfloat16)
        gate_value = jax.nn.sigmoid(jnp.dot(flattened, gate_weight, preferred_element_type=jnp.float32)).reshape(RES_DEV, N, C)
        return (left_proj, right_proj, gate_value)
    blocks = pair_map.reshape(N // RES_DEV, RES_DEV, N, C)
    mask_blocks = mask_float.reshape(N // RES_DEV, RES_DEV)
    left_proj, right_proj, gate_value = lax.map(project, (blocks, mask_blocks))
    right_wide = right_proj.reshape(N, N, HID).astype(jnp.float32)

    def finish(inputs):
        left_block, gate_block = inputs
        triangle = jnp.einsum('ikc,jkc->ijc', left_block.astype(jnp.float32), right_wide).astype(jnp.bfloat16)
        normed_tri = layer_norm(triangle.astype(jnp.float32)).astype(jnp.bfloat16)
        mixed_out = jnp.dot(normed_tri.reshape(-1, HID), out_weight, preferred_element_type=jnp.float32).reshape(RES_DEV, N, C)
        return (gate_block * mixed_out).astype(jnp.bfloat16)
    update = lax.map(finish, (left_proj, gate_value))
    return update.reshape(N, N, C)
```

```python
import functools

import jax
import jax.numpy as jnp
from jax import lax
from jax.experimental import pallas as pl
from jax.experimental.pallas import tpu as pltpu
from jax.sharding import PartitionSpec as P

epsilon = 1.0


def partner_2(x, axis, bit):
    return lax.ppermute(x, axis, [(i, i ^ 1 << bit) for i in range(lax.axis_size(axis))])


def layer_norm_lead(values):
    average = jnp.mean(values, axis=0, keepdims=True)
    centred = values - average
    variance = jnp.mean(centred * centred, axis=0, keepdims=True)
    return centred * lax.rsqrt(variance + epsilon)


def layer_norm_last(values):
    average = jnp.mean(values, axis=-1, keepdims=True)
    centred = values - average
    variance = jnp.mean(centred * centred, axis=-1, keepdims=True)
    return centred * lax.rsqrt(variance + epsilon)


def swap_with(values, bit):
    return partner_2(values, "gx", bit)


def pair_join(values, bit, position):
    partner = swap_with(values, bit)
    mine_first = position // 2**bit % 2 == 0
    return jnp.where(
        mine_first,
        jnp.concatenate([values, partner], axis=1),
        jnp.concatenate([partner, values], axis=1),
    )


def whole_channels(gathered, out_weight, gate_value):
    hidden, row_count, col_count = gathered.shape
    normed_tri = layer_norm_lead(gathered.astype(jnp.float32)).astype(jnp.bfloat16)
    mixed_out = lax.dot_general(
        normed_tri.reshape(hidden, row_count * col_count),
        out_weight,
        (((0,), (0,)), ((), ())),
        preferred_element_type=jnp.float32,
    )
    return gate_value * mixed_out.reshape(row_count, col_count, out_weight.shape[1])


def local(pair_map, residue_mask, proj_weight, gate_weight, out_weight):
    row_count, col_count, chan_count = pair_map.shape
    hidden = out_weight.shape[0]
    residues = residue_mask.shape[0]
    along_x = lax.axis_size("gx")
    along_y = lax.axis_size("gy")
    along_z = lax.axis_size("gz")
    mask_float = residue_mask.astype(jnp.float32)
    row_mask = lax.dynamic_slice_in_dim(mask_float, lax.axis_index("gx") * row_count, row_count)
    col_mask = lax.dynamic_slice_in_dim(
        mask_float, (lax.axis_index("gy") * along_z + lax.axis_index("gz")) * col_count, col_count
    )
    normed = layer_norm_last(pair_map.astype(jnp.float32)).astype(jnp.bfloat16)
    flattened = normed.reshape(row_count * col_count, chan_count)
    projected = lax.dot_general(
        proj_weight, flattened, (((0,), (1,)), ((), ())), preferred_element_type=jnp.float32
    ).reshape(4 * hidden, row_count, col_count)
    pair_mask = (row_mask[:, None] * col_mask[None, :])[None, :, :]
    left_proj = (
        jax.nn.sigmoid(projected[:hidden]) * projected[hidden : 2 * hidden] * pair_mask
    ).astype(jnp.bfloat16)
    right_proj = (
        jax.nn.sigmoid(projected[2 * hidden : 3 * hidden]) * projected[3 * hidden :] * pair_mask
    ).astype(jnp.bfloat16)
    gate_value = jax.nn.sigmoid(
        jnp.dot(flattened, gate_weight, preferred_element_type=jnp.float32)
    ).reshape(row_count, col_count, chan_count)
    group_count = along_y * along_z
    group_chan = hidden // group_count
    left_group, right_group = (
        lax.all_to_all(left_proj, ("gy", "gz"), split_axis=0, concat_axis=2, tiled=True),
        lax.all_to_all(right_proj, ("gy", "gz"), split_axis=0, concat_axis=2, tiled=True),
    )
    levels = along_x.bit_length() - 1
    low_bits = levels // 2
    high_count = 2 ** (levels - low_bits)
    low_count = 2**low_bits
    position = lax.axis_index("gx")
    left_tile = left_group
    for bit in range(low_bits):
        left_tile = pair_join(left_tile, bit, position)
    right_tile = right_group
    for bit in range(low_bits, levels):
        right_tile = pair_join(right_tile, bit, position)
    block_tile = jnp.einsum(
        "cik,cjk->cij", left_tile, right_tile, preferred_element_type=jnp.float32
    ).astype(jnp.bfloat16)
    for bit in range(low_bits):
        current = block_tile.shape[1]
        span = block_tile.shape[2]
        shaped = block_tile.reshape(group_chan, current // (2 * row_count), 2, row_count, span)
        own_bit = position // 2**bit % 2
        kept = lax.dynamic_index_in_dim(shaped, own_bit, axis=2, keepdims=False).reshape(
            group_chan, current // 2, span
        )
        sent = lax.dynamic_index_in_dim(shaped, 1 - own_bit, axis=2, keepdims=False).reshape(
            group_chan, current // 2, span
        )
        arrived = swap_with(sent, bit)
        block_tile = jnp.where(
            own_bit == 0,
            jnp.concatenate([kept, arrived], axis=2),
            jnp.concatenate([arrived, kept], axis=2),
        )
    block_tile = (
        block_tile.reshape(group_chan, row_count, low_count, high_count, row_count)
        .transpose(0, 1, 3, 2, 4)
        .reshape(group_chan, row_count, residues)
    )
    gathered = lax.all_to_all(block_tile, ("gy", "gz"), split_axis=2, concat_axis=0, tiled=True)
    update = whole_channels(gathered, out_weight, gate_value)
    return update.astype(jnp.bfloat16)


MESH = pl.DeviceIdType.MESH
LANES = 128
VMEM_BUDGET = 48 * 2**20


def up(value, step):
    return -(-value // step) * step


def fused_kernel(
    along_y, along_z,
    pair_ref, mask_ref, proj_ref, gate_ref, out_w_ref, out_ref,
    rows_f32, normed_bf, masked_bf, gate_f32, send_a, recv_a, recv_x, left_s, right_s, tri_s, send_b, recv_b,
    ssem_a, rsem_a, ssem_x, rsem_x, ssem_b, rsem_b, own_sem,
):
    rows, cols, chans = pair_ref.shape
    hidden = out_w_ref.shape[0]
    groups = along_y * along_z
    gc = hidden // groups
    pad = rows_f32.shape[0] // rows
    flat = rows * cols
    residues = mask_ref.shape[1]
    px, py, pz = lax.axis_index("gx"), lax.axis_index("gy"), lax.axis_index("gz")
    me = py * along_z + pz

    def place(d):
        return (px, d // along_z, d % along_z)

    partner = (1 - px, py, pz)
    barrier = pltpu.get_barrier_semaphore()

    def greet(o, carry):
        pl.semaphore_signal(barrier, inc=1, device_id=place((me + o) % groups), device_id_type=MESH)
        return carry

    lax.fori_loop(1, groups, greet, 0)
    pl.semaphore_signal(barrier, inc=1, device_id=partner, device_id_type=MESH)

    for i in range(rows):
        rows_f32[pl.ds(i * pad, cols), :] = pair_ref[i].astype(jnp.float32)
    mask_f = mask_ref[...].astype(jnp.float32)
    lane = lax.broadcasted_iota(jnp.int32, (rows, residues), 1)
    sub = lax.broadcasted_iota(jnp.int32, (rows, residues), 0)
    row_mask = jnp.sum(jnp.where(lane == sub + px * rows, mask_f, 0.0), axis=1, keepdims=True)
    lane_row = lax.broadcasted_iota(jnp.int32, (1, residues), 1)
    for k in range(cols):
        col_mask = jnp.sum(
            jnp.where(lane_row == me * cols + k, mask_f, 0.0), axis=1, keepdims=True
        )
        normed = layer_norm_last(rows_f32[pl.ds(k, rows, stride=pad), :]).astype(jnp.bfloat16)
        normed_bf[k * rows : (k + 1) * rows, :] = normed
        masked_bf[k * rows : (k + 1) * rows, :] = (
            normed.astype(jnp.float32) * (row_mask * col_mask)
        ).astype(jnp.bfloat16)

    proj_t = proj_ref[...].astype(jnp.float32).T.astype(jnp.bfloat16)
    masked = masked_bf[...]

    def project(first, count):
        return lax.dot_general(
            proj_t[first : first + count], masked, (((1,), (1,)), ((), ())),
            preferred_element_type=jnp.float32,
        )

    step = 4 * gc
    for first in range(0, hidden, step):
        for side in range(2):
            base = 2 * side * hidden + first
            value = jax.nn.sigmoid(project(base, step)) * project(base + hidden, step)
            for part in range(step // gc):
                send_a[first // gc + part, side, :, 0:flat] = value[
                    part * gc : (part + 1) * gc
                ].astype(jnp.bfloat16)

    def copy_a(d, slot):
        return pltpu.make_async_remote_copy(
            src_ref=send_a.at[d], dst_ref=recv_a.at[slot], send_sem=ssem_a.at[d],
            recv_sem=rsem_a.at[slot], device_id=place(d), device_id_type=MESH,
        )

    def copy_x(s):
        return pltpu.make_async_remote_copy(
            src_ref=recv_a.at[s, 1], dst_ref=recv_x.at[s], send_sem=ssem_x.at[s],
            recv_sem=rsem_x.at[s], device_id=partner, device_id_type=MESH,
        )

    def copy_b(d, slot):
        return pltpu.make_async_remote_copy(
            src_ref=send_b.at[d], dst_ref=recv_b.at[slot], send_sem=ssem_b.at[d],
            recv_sem=rsem_b.at[slot], device_id=place(d), device_id_type=MESH,
        )

    pl.semaphore_wait(barrier, groups)

    def start_a(o, carry):
        copy_a((me + o) % groups, me).start()
        return carry

    lax.fori_loop(1, groups, start_a, 0)
    own_a = pltpu.make_async_copy(send_a.at[me], recv_a.at[me], own_sem.at[0])
    own_a.start()

    gate_f32[...] = jax.nn.sigmoid(
        jnp.dot(normed_bf[...], gate_ref[...], preferred_element_type=jnp.float32)
    )

    def spread(value, target, s):
        value = value.astype(jnp.float32)
        for k in range(cols):
            at = pl.multiple_of((s * cols + k) * gc, gc)
            target[pl.ds(at, gc), 0:rows] = value[:, k * rows : (k + 1) * rows]

    def take(s):
        copy_x(s).start()
        spread(recv_a[s, 0], left_s, s)
        spread(recv_a[s, 1], right_s.at[px], s)

    own_a.wait()
    take(me)

    def take_a(o, carry):
        s = (me + groups - o) % groups
        copy_a(s, s).wait_recv()
        take(s)
        return carry

    lax.fori_loop(1, groups, take_a, 0)

    def take_x(o, carry):
        s = (me + groups - o) % groups
        copy_x(s).wait_recv()
        spread(recv_x[s], right_s.at[1 - px], s)
        return carry

    lax.fori_loop(0, groups, take_x, 0)

    for c in range(gc):
        left = left_s[pl.ds(c, residues, stride=gc), :].astype(jnp.bfloat16)
        for half in range(2):
            right = right_s[half, pl.ds(c, residues, stride=gc), :].astype(jnp.bfloat16)
            block = lax.dot_general(
                right, left, (((0,), (0,)), ((), ())), preferred_element_type=jnp.float32
            )
            tri_s[pl.ds(half * rows * gc + c, rows, stride=gc), :] = block[0:rows]

    def start_b(o, carry):
        d = (me + o) % groups
        pieces = []
        for j in range(cols):
            at = pl.multiple_of((d * cols + j) * gc, gc)
            pieces.append(tri_s[pl.ds(at, gc), 0:rows])
        send_b[d, :, 0:flat] = jnp.concatenate(pieces, axis=1).astype(jnp.bfloat16)

        @pl.when(o < groups)
        def _():
            copy_b(d, me).start()

        return carry

    lax.fori_loop(1, groups + 1, start_b, 0)
    own_b = pltpu.make_async_copy(send_b.at[me], recv_b.at[me], own_sem.at[1])
    own_b.start()
    own_b.wait()

    def take_b(o, carry):
        s = (me + groups - o) % groups
        copy_b(s, s).wait_recv()
        return carry

    lax.fori_loop(1, groups, take_b, 0)

    triangle = recv_b[:, :, 0:flat].astype(jnp.float32).reshape(hidden, flat)
    normed_tri = layer_norm_lead(triangle).astype(jnp.bfloat16)
    mixed = lax.dot_general(
        normed_tri, out_w_ref[...], (((0,), (0,)), ((), ())), preferred_element_type=jnp.float32
    )
    update = gate_f32[...] * mixed
    for j in range(cols):
        rows_f32[pl.ds(j, rows, stride=pad), :] = update[j * rows : (j + 1) * rows]
    for i in range(rows):
        out_ref[i] = rows_f32[pl.ds(i * pad, cols), :].astype(jnp.bfloat16)

    def finish(o, carry):
        d = (me + o) % groups
        copy_a(d, me).wait_send()
        copy_b(d, me).wait_send()
        return carry

    lax.fori_loop(1, groups, finish, 0)

    def finish_x(s, carry):
        copy_x(s).wait_send()
        return carry

    lax.fori_loop(0, groups, finish_x, 0)


def scratch_list(rows, cols, chans, hidden, groups, residues):
    gc = hidden // groups
    flat = up(rows * cols, LANES)
    pad = up(cols, 8)
    bf, f32 = jnp.bfloat16, jnp.float32
    return [
        ((rows * pad, chans), f32),
        ((rows * cols, chans), bf),
        ((rows * cols, chans), bf),
        ((rows * cols, chans), f32),
        ((groups, 2, gc, flat), bf),
        ((groups, 2, gc, flat), bf),
        ((groups, gc, flat), bf),
        ((residues * gc, LANES), f32),
        ((2, residues * gc, LANES), f32),
        ((residues * gc, LANES), f32),
        ((groups, gc, flat), bf),
        ((groups, gc, flat), bf),
    ]


def fits_kernel(sizes, rows, cols, chans, hidden, residues):
    groups = sizes["gy"] * sizes["gz"]
    if sizes["gx"] != 2 or hidden % (4 * groups) or hidden // groups != 8:
        return False
    if chans != LANES or rows > LANES or rows % 16:
        return False
    total = 0
    for shape, kind in scratch_list(rows, cols, chans, hidden, groups, residues):
        count = 1
        for extent in shape:
            count *= extent
        total += count * jnp.dtype(kind).itemsize
    return total < VMEM_BUDGET // 4


def local_fused(sizes, pair_map, residue_mask, proj_weight, gate_weight, out_weight):
    rows, cols, chans = pair_map.shape
    hidden = out_weight.shape[0]
    residues = residue_mask.shape[0]
    if not fits_kernel(sizes, rows, cols, chans, hidden, residues):
        return local(pair_map, residue_mask, proj_weight, gate_weight, out_weight)
    groups = sizes["gy"] * sizes["gz"]
    dma = pltpu.SemaphoreType.DMA((groups,))
    vmem = pl.BlockSpec(memory_space=pltpu.VMEM)
    return pl.pallas_call(
        functools.partial(fused_kernel, sizes["gy"], sizes["gz"]),
        out_shape=jax.ShapeDtypeStruct(pair_map.shape, jnp.bfloat16),
        in_specs=[vmem] * 5,
        out_specs=vmem,
        scratch_shapes=[
            pltpu.VMEM(shape, kind)
            for shape, kind in scratch_list(rows, cols, chans, hidden, groups, residues)
        ]
        + [dma] * 6
        + [pltpu.SemaphoreType.DMA((2,))],
        compiler_params=pltpu.CompilerParams(
            collective_id=0, has_side_effects=True, vmem_limit_bytes=VMEM_BUDGET
        ),
    )(pair_map, residue_mask.reshape(1, residues), proj_weight, gate_weight, out_weight)


def solution(mesh):
    placed = (P("gx", ("gy", "gz"), None), P(), P(), P(), P())
    return jax.shard_map(
        functools.partial(local_fused, dict(mesh.shape)), mesh=mesh, in_specs=placed, out_specs=P("gx", ("gy", "gz"), None), check_vma=False
    )
```

```python
import functools

import jax
import jax.numpy as jnp
from jax import lax
from jax.experimental import pallas as pl
from jax.experimental.pallas import tpu as pltpu
from jax.sharding import PartitionSpec as P

epsilon = 1.0


def partner_2(x, axis, bit):
    return lax.ppermute(x, axis, [(i, i ^ 1 << bit) for i in range(lax.axis_size(axis))])


def layer_norm_lead(values):
    average = jnp.mean(values, axis=0, keepdims=True)
    centred = values - average
    variance = jnp.mean(centred * centred, axis=0, keepdims=True)
    return centred * lax.rsqrt(variance + epsilon)


def layer_norm_last(values):
    average = jnp.mean(values, axis=-1, keepdims=True)
    centred = values - average
    variance = jnp.mean(centred * centred, axis=-1, keepdims=True)
    return centred * lax.rsqrt(variance + epsilon)


def swap_with(values, bit):
    return partner_2(values, "gx", bit)


def pair_join(values, bit, position):
    partner = swap_with(values, bit)
    mine_first = position // 2**bit % 2 == 0
    return jnp.where(
        mine_first,
        jnp.concatenate([values, partner], axis=1),
        jnp.concatenate([partner, values], axis=1),
    )


def whole_channels(gathered, out_weight, gate_value):
    hidden, row_count, col_count = gathered.shape
    normed_tri = layer_norm_lead(gathered.astype(jnp.float32)).astype(jnp.bfloat16)
    mixed_out = lax.dot_general(
        normed_tri.reshape(hidden, row_count * col_count),
        out_weight,
        (((0,), (0,)), ((), ())),
        preferred_element_type=jnp.float32,
    )
    return gate_value * mixed_out.reshape(row_count, col_count, out_weight.shape[1])


def local(pair_map, residue_mask, proj_weight, gate_weight, out_weight):
    row_count, col_count, chan_count = pair_map.shape
    hidden = out_weight.shape[0]
    residues = residue_mask.shape[0]
    along_x = lax.axis_size("gx")
    along_y = lax.axis_size("gy")
    along_z = lax.axis_size("gz")
    mask_float = residue_mask.astype(jnp.float32)
    row_mask = lax.dynamic_slice_in_dim(mask_float, lax.axis_index("gx") * row_count, row_count)
    col_mask = lax.dynamic_slice_in_dim(
        mask_float, (lax.axis_index("gy") * along_z + lax.axis_index("gz")) * col_count, col_count
    )
    normed = layer_norm_last(pair_map.astype(jnp.float32)).astype(jnp.bfloat16)
    flattened = normed.reshape(row_count * col_count, chan_count)
    projected = lax.dot_general(
        proj_weight, flattened, (((0,), (1,)), ((), ())), preferred_element_type=jnp.float32
    ).reshape(4 * hidden, row_count, col_count)
    pair_mask = (row_mask[:, None] * col_mask[None, :])[None, :, :]
    left_proj = (
        jax.nn.sigmoid(projected[:hidden]) * projected[hidden : 2 * hidden] * pair_mask
    ).astype(jnp.bfloat16)
    right_proj = (
        jax.nn.sigmoid(projected[2 * hidden : 3 * hidden]) * projected[3 * hidden :] * pair_mask
    ).astype(jnp.bfloat16)
    gate_value = jax.nn.sigmoid(
        jnp.dot(flattened, gate_weight, preferred_element_type=jnp.float32)
    ).reshape(row_count, col_count, chan_count)
    group_count = along_y * along_z
    group_chan = hidden // group_count
    left_group, right_group = (
        lax.all_to_all(left_proj, ("gy", "gz"), split_axis=0, concat_axis=2, tiled=True),
        lax.all_to_all(right_proj, ("gy", "gz"), split_axis=0, concat_axis=2, tiled=True),
    )
    levels = along_x.bit_length() - 1
    low_bits = levels // 2
    high_count = 2 ** (levels - low_bits)
    low_count = 2**low_bits
    position = lax.axis_index("gx")
    left_tile = left_group
    for bit in range(low_bits):
        left_tile = pair_join(left_tile, bit, position)
    right_tile = right_group
    for bit in range(low_bits, levels):
        right_tile = pair_join(right_tile, bit, position)
    block_tile = jnp.einsum(
        "cik,cjk->cij", left_tile, right_tile, preferred_element_type=jnp.float32
    ).astype(jnp.bfloat16)
    for bit in range(low_bits):
        current = block_tile.shape[1]
        span = block_tile.shape[2]
        shaped = block_tile.reshape(group_chan, current // (2 * row_count), 2, row_count, span)
        own_bit = position // 2**bit % 2
        kept = lax.dynamic_index_in_dim(shaped, own_bit, axis=2, keepdims=False).reshape(
            group_chan, current // 2, span
        )
        sent = lax.dynamic_index_in_dim(shaped, 1 - own_bit, axis=2, keepdims=False).reshape(
            group_chan, current // 2, span
        )
        arrived = swap_with(sent, bit)
        block_tile = jnp.where(
            own_bit == 0,
            jnp.concatenate([kept, arrived], axis=2),
            jnp.concatenate([arrived, kept], axis=2),
        )
    block_tile = (
        block_tile.reshape(group_chan, row_count, low_count, high_count, row_count)
        .transpose(0, 1, 3, 2, 4)
        .reshape(group_chan, row_count, residues)
    )
    gathered = lax.all_to_all(block_tile, ("gy", "gz"), split_axis=2, concat_axis=0, tiled=True)
    update = whole_channels(gathered, out_weight, gate_value)
    return update.astype(jnp.bfloat16)


MESH = pl.DeviceIdType.MESH
LANES = 128
VMEM_BUDGET = 48 * 2**20


def up(value, step):
    return -(-value // step) * step


def fused_kernel(
    along_y, along_z,
    pair_ref, mask_ref, proj_ref, gate_ref, out_w_ref, out_ref,
    normed_bf, masked_bf, gate_f32, send_r, recv_r, recv_x, send_l, recv_l,
    left_s, right_s, tri_s, send_b, recv_b,
    ssem_r, rsem_r, ssem_x, rsem_x, ssem_l, rsem_l, ssem_b, rsem_b, own_sem,
):
    cols, rows, chans = pair_ref.shape
    hidden = out_w_ref.shape[0]
    groups = along_y * along_z
    gc = hidden // groups
    hc = gc // 2
    flat = rows * cols
    residues = mask_ref.shape[1]
    px, py, pz = lax.axis_index("gx"), lax.axis_index("gy"), lax.axis_index("gz")
    me = py * along_z + pz

    def place(d):
        return (px, d // along_z, d % along_z)

    partner = (1 - px, py, pz)
    barrier = pltpu.get_barrier_semaphore()

    def greet(o, carry):
        pl.semaphore_signal(barrier, inc=1, device_id=place((me + o) % groups), device_id_type=MESH)
        return carry

    lax.fori_loop(1, groups, greet, 0)
    pl.semaphore_signal(barrier, inc=1, device_id=partner, device_id_type=MESH)

    mask_f = mask_ref[...].astype(jnp.float32)
    lane = lax.broadcasted_iota(jnp.int32, (rows, residues), 1)
    sub = lax.broadcasted_iota(jnp.int32, (rows, residues), 0)
    row_mask = jnp.sum(jnp.where(lane == sub + px * rows, mask_f, 0.0), axis=1, keepdims=True)
    lane_row = lax.broadcasted_iota(jnp.int32, (1, residues), 1)
    for k in range(cols):
        col_mask = jnp.sum(
            jnp.where(lane_row == me * cols + k, mask_f, 0.0), axis=1, keepdims=True
        )
        normed = layer_norm_last(pair_ref[k].astype(jnp.float32)).astype(jnp.bfloat16)
        normed_bf[k * rows : (k + 1) * rows, :] = normed
        masked_bf[k * rows : (k + 1) * rows, :] = (
            normed.astype(jnp.float32) * (row_mask * col_mask)
        ).astype(jnp.bfloat16)

    proj_t = proj_ref[...].astype(jnp.float32).T.astype(jnp.bfloat16)
    masked = masked_bf[...]

    def project(first, count):
        return lax.dot_general(
            proj_t[first : first + count], masked, (((1,), (1,)), ((), ())),
            preferred_element_type=jnp.float32,
        )

    def copy_r(d, slot):
        return pltpu.make_async_remote_copy(
            src_ref=send_r.at[d], dst_ref=recv_r.at[slot], send_sem=ssem_r.at[d],
            recv_sem=rsem_r.at[slot], device_id=place(d), device_id_type=MESH,
        )

    def copy_l(h, d, slot):
        return pltpu.make_async_remote_copy(
            src_ref=send_l.at[h, d], dst_ref=recv_l.at[h, slot], send_sem=ssem_l.at[h, d],
            recv_sem=rsem_l.at[h, slot], device_id=place(d), device_id_type=MESH,
        )

    def copy_x(s):
        return pltpu.make_async_remote_copy(
            src_ref=recv_r.at[s], dst_ref=recv_x.at[s], send_sem=ssem_x.at[s],
            recv_sem=rsem_x.at[s], device_id=partner, device_id_type=MESH,
        )

    def copy_b(h, d, slot):
        return pltpu.make_async_remote_copy(
            src_ref=send_b.at[h, d], dst_ref=recv_b.at[h, slot], send_sem=ssem_b.at[h, d],
            recv_sem=rsem_b.at[h, slot], device_id=place(d), device_id_type=MESH,
        )

    step = 4 * gc

    def gated(first, side):
        base = 2 * side * hidden + first
        return jax.nn.sigmoid(project(base, step)) * project(base + hidden, step)

    for first in range(0, hidden, step):
        value = gated(first, 1)
        for part in range(step // gc):
            send_r[first // gc + part, :, 0:flat] = value[
                part * gc : (part + 1) * gc
            ].astype(jnp.bfloat16)

    pl.semaphore_wait(barrier, groups)

    def start_r(o, carry):
        copy_r((me + o) % groups, me).start()
        return carry

    lax.fori_loop(1, groups, start_r, 0)
    own_r = pltpu.make_async_copy(send_r.at[me], recv_r.at[me], own_sem.at[0])
    own_r.start()

    for first in range(0, hidden, step):
        value = gated(first, 0)
        for part in range(step // gc):
            for h in range(2):
                low = part * gc + h * hc
                send_l[h, first // gc + part, :, 0:flat] = value[low : low + hc].astype(jnp.bfloat16)

    for h in range(2):

        def start_l(o, carry, h=h):
            copy_l(h, (me + o) % groups, me).start()
            return carry

        lax.fori_loop(1, groups, start_l, 0)

    gate_f32[...] = jax.nn.sigmoid(
        jnp.dot(normed_bf[...], gate_ref[...], preferred_element_type=jnp.float32)
    )

    def spread(value, target, s, first, count):
        value = value.astype(jnp.float32)
        for k in range(cols):
            at = pl.multiple_of((s * cols + k) * gc, gc)
            target[pl.ds(at + first, count), 0:rows] = value[:, k * rows : (k + 1) * rows]

    own_r.wait()

    def take_r(o, carry):
        s = (me + groups - o) % groups

        @pl.when(o > 0)
        def _():
            copy_r(s, s).wait_recv()

        copy_x(s).start()
        spread(recv_r[s], right_s.at[px], s, 0, gc)
        return carry

    lax.fori_loop(0, groups, take_r, 0)

    def take_x(o, carry):
        s = (me + groups - o) % groups
        copy_x(s).wait_recv()
        spread(recv_x[s], right_s.at[1 - px], s, 0, gc)
        return carry

    lax.fori_loop(0, groups, take_x, 0)

    for h in range(2):
        spread(send_l[h, me], left_s, me, h * hc, hc)

        def take_l(o, carry, h=h):
            s = (me + groups - o) % groups
            copy_l(h, s, s).wait_recv()
            spread(recv_l[h, s], left_s, s, h * hc, hc)
            return carry

        lax.fori_loop(1, groups, take_l, 0)

        for c in range(h * hc, (h + 1) * hc):
            left = left_s[pl.ds(c, residues, stride=gc), :].astype(jnp.bfloat16)
            for half in range(2):
                right = right_s[half, pl.ds(c, residues, stride=gc), :].astype(jnp.bfloat16)
                block = lax.dot_general(
                    right, left, (((0,), (0,)), ((), ())), preferred_element_type=jnp.float32
                )
                tri_s[pl.ds(half * rows * gc + c, rows, stride=gc), :] = block[0:rows]

        def pack_b(d, h=h):
            pieces = []
            for j in range(cols):
                at = pl.multiple_of((d * cols + j) * gc, gc)
                pieces.append(tri_s[pl.ds(at + h * hc, hc), 0:rows])
            return jnp.concatenate(pieces, axis=1).astype(jnp.bfloat16)

        def start_b(o, carry, h=h):
            d = (me + o) % groups
            send_b[h, d, :, 0:flat] = pack_b(d)
            copy_b(h, d, me).start()
            return carry

        lax.fori_loop(1, groups, start_b, 0)
        recv_b[h, me, :, 0:flat] = pack_b(me)

    for h in range(2):

        def take_b(o, carry, h=h):
            s = (me + groups - o) % groups
            copy_b(h, s, s).wait_recv()
            return carry

        lax.fori_loop(1, groups, take_b, 0)

    triangle = jnp.concatenate(
        [recv_b[h, :, :, 0:flat].astype(jnp.float32) for h in range(2)], axis=1
    ).reshape(hidden, flat)
    normed_tri = layer_norm_lead(triangle).astype(jnp.bfloat16)
    mixed = lax.dot_general(
        normed_tri, out_w_ref[...], (((0,), (0,)), ((), ())), preferred_element_type=jnp.float32
    )
    update = gate_f32[...] * mixed
    for j in range(cols):
        out_ref[j] = update[j * rows : (j + 1) * rows].astype(jnp.bfloat16)

    def finish(o, carry):
        d = (me + o) % groups
        copy_r(d, me).wait_send()
        for h in range(2):
            copy_l(h, d, me).wait_send()
            copy_b(h, d, me).wait_send()
        return carry

    lax.fori_loop(1, groups, finish, 0)

    def finish_x(s, carry):
        copy_x(s).wait_send()
        return carry

    lax.fori_loop(0, groups, finish_x, 0)


def scratch_list(rows, cols, chans, hidden, groups, residues):
    gc = hidden // groups
    flat = up(rows * cols, LANES)
    hc = gc // 2
    bf, f32 = jnp.bfloat16, jnp.float32
    return [
        ((rows * cols, chans), bf),
        ((rows * cols, chans), bf),
        ((rows * cols, chans), f32),
        ((groups, gc, flat), bf),
        ((groups, gc, flat), bf),
        ((groups, gc, flat), bf),
        ((2, groups, hc, flat), bf),
        ((2, groups, hc, flat), bf),
        ((residues * gc, LANES), f32),
        ((2, residues * gc, LANES), f32),
        ((residues * gc, LANES), f32),
        ((2, groups, hc, flat), bf),
        ((2, groups, hc, flat), bf),
    ]


def fits_kernel(sizes, rows, cols, chans, hidden, residues):
    groups = sizes["gy"] * sizes["gz"]
    if sizes["gx"] != 2 or hidden % (4 * groups) or hidden // groups != 8:
        return False
    if chans != LANES or rows > LANES or rows % 16:
        return False
    total = 0
    for shape, kind in scratch_list(rows, cols, chans, hidden, groups, residues):
        count = 1
        for extent in shape:
            count *= extent
        total += count * jnp.dtype(kind).itemsize
    return total < VMEM_BUDGET // 4


def local_fused(sizes, pair_map, residue_mask, proj_weight, gate_weight, out_weight):
    rows, cols, chans = pair_map.shape
    hidden = out_weight.shape[0]
    residues = residue_mask.shape[0]
    if not fits_kernel(sizes, rows, cols, chans, hidden, residues):
        return local(pair_map, residue_mask, proj_weight, gate_weight, out_weight)
    groups = sizes["gy"] * sizes["gz"]
    dma = pltpu.SemaphoreType.DMA((groups,))
    dma_halves = pltpu.SemaphoreType.DMA((2, groups))
    vmem = pl.BlockSpec(memory_space=pltpu.VMEM)
    turned = pl.pallas_call(
        functools.partial(fused_kernel, sizes["gy"], sizes["gz"]),
        out_shape=jax.ShapeDtypeStruct((cols, rows, chans), jnp.bfloat16),
        in_specs=[vmem] * 5,
        out_specs=vmem,
        scratch_shapes=[
            pltpu.VMEM(shape, kind)
            for shape, kind in scratch_list(rows, cols, chans, hidden, groups, residues)
        ]
        + [dma] * 4
        + [dma_halves] * 4
        + [pltpu.SemaphoreType.DMA((1,))],
        compiler_params=pltpu.CompilerParams(
            collective_id=0, has_side_effects=True, vmem_limit_bytes=VMEM_BUDGET
        ),
    )(
        pair_map.transpose(1, 0, 2), residue_mask.reshape(1, residues),
        proj_weight, gate_weight, out_weight,
    )
    return turned.transpose(1, 0, 2)


def solution(mesh):
    placed = (P("gx", ("gy", "gz"), None), P(), P(), P(), P())
    return jax.shard_map(
        functools.partial(local_fused, dict(mesh.shape)), mesh=mesh, in_specs=placed, out_specs=P("gx", ("gy", "gz"), None), check_vma=False
    )
```

```python
import functools

import jax
import jax.numpy as jnp
from jax import lax
from jax.experimental import pallas as pl
from jax.experimental.pallas import tpu as pltpu
from jax.sharding import PartitionSpec as P

epsilon = 1.0


def partner_2(x, axis, bit):
    return lax.ppermute(x, axis, [(i, i ^ 1 << bit) for i in range(lax.axis_size(axis))])


def layer_norm_lead(values):
    average = jnp.mean(values, axis=0, keepdims=True)
    centred = values - average
    variance = jnp.mean(centred * centred, axis=0, keepdims=True)
    return centred * lax.rsqrt(variance + epsilon)


def layer_norm_last(values):
    average = jnp.mean(values, axis=-1, keepdims=True)
    centred = values - average
    variance = jnp.mean(centred * centred, axis=-1, keepdims=True)
    return centred * lax.rsqrt(variance + epsilon)


def swap_with(values, bit):
    return partner_2(values, "gx", bit)


def pair_join(values, bit, position):
    partner = swap_with(values, bit)
    mine_first = position // 2**bit % 2 == 0
    return jnp.where(
        mine_first,
        jnp.concatenate([values, partner], axis=1),
        jnp.concatenate([partner, values], axis=1),
    )


def whole_channels(gathered, out_weight, gate_value):
    hidden, row_count, col_count = gathered.shape
    normed_tri = layer_norm_lead(gathered.astype(jnp.float32)).astype(jnp.bfloat16)
    mixed_out = lax.dot_general(
        normed_tri.reshape(hidden, row_count * col_count),
        out_weight,
        (((0,), (0,)), ((), ())),
        preferred_element_type=jnp.float32,
    )
    return gate_value * mixed_out.reshape(row_count, col_count, out_weight.shape[1])


def local(pair_map, residue_mask, proj_weight, gate_weight, out_weight):
    row_count, col_count, chan_count = pair_map.shape
    hidden = out_weight.shape[0]
    residues = residue_mask.shape[0]
    along_x = lax.axis_size("gx")
    along_y = lax.axis_size("gy")
    along_z = lax.axis_size("gz")
    mask_float = residue_mask.astype(jnp.float32)
    row_mask = lax.dynamic_slice_in_dim(mask_float, lax.axis_index("gx") * row_count, row_count)
    col_mask = lax.dynamic_slice_in_dim(
        mask_float, (lax.axis_index("gy") * along_z + lax.axis_index("gz")) * col_count, col_count
    )
    normed = layer_norm_last(pair_map.astype(jnp.float32)).astype(jnp.bfloat16)
    flattened = normed.reshape(row_count * col_count, chan_count)
    projected = lax.dot_general(
        proj_weight, flattened, (((0,), (1,)), ((), ())), preferred_element_type=jnp.float32
    ).reshape(4 * hidden, row_count, col_count)
    pair_mask = (row_mask[:, None] * col_mask[None, :])[None, :, :]
    left_proj = (
        jax.nn.sigmoid(projected[:hidden]) * projected[hidden : 2 * hidden] * pair_mask
    ).astype(jnp.bfloat16)
    right_proj = (
        jax.nn.sigmoid(projected[2 * hidden : 3 * hidden]) * projected[3 * hidden :] * pair_mask
    ).astype(jnp.bfloat16)
    gate_value = jax.nn.sigmoid(
        jnp.dot(flattened, gate_weight, preferred_element_type=jnp.float32)
    ).reshape(row_count, col_count, chan_count)
    group_count = along_y * along_z
    group_chan = hidden // group_count
    left_group, right_group = (
        lax.all_to_all(left_proj, ("gy", "gz"), split_axis=0, concat_axis=2, tiled=True),
        lax.all_to_all(right_proj, ("gy", "gz"), split_axis=0, concat_axis=2, tiled=True),
    )
    levels = along_x.bit_length() - 1
    low_bits = levels // 2
    high_count = 2 ** (levels - low_bits)
    low_count = 2**low_bits
    position = lax.axis_index("gx")
    left_tile = left_group
    for bit in range(low_bits):
        left_tile = pair_join(left_tile, bit, position)
    right_tile = right_group
    for bit in range(low_bits, levels):
        right_tile = pair_join(right_tile, bit, position)
    block_tile = jnp.einsum(
        "cik,cjk->cij", left_tile, right_tile, preferred_element_type=jnp.float32
    ).astype(jnp.bfloat16)
    for bit in range(low_bits):
        current = block_tile.shape[1]
        span = block_tile.shape[2]
        shaped = block_tile.reshape(group_chan, current // (2 * row_count), 2, row_count, span)
        own_bit = position // 2**bit % 2
        kept = lax.dynamic_index_in_dim(shaped, own_bit, axis=2, keepdims=False).reshape(
            group_chan, current // 2, span
        )
        sent = lax.dynamic_index_in_dim(shaped, 1 - own_bit, axis=2, keepdims=False).reshape(
            group_chan, current // 2, span
        )
        arrived = swap_with(sent, bit)
        block_tile = jnp.where(
            own_bit == 0,
            jnp.concatenate([kept, arrived], axis=2),
            jnp.concatenate([arrived, kept], axis=2),
        )
    block_tile = (
        block_tile.reshape(group_chan, row_count, low_count, high_count, row_count)
        .transpose(0, 1, 3, 2, 4)
        .reshape(group_chan, row_count, residues)
    )
    gathered = lax.all_to_all(block_tile, ("gy", "gz"), split_axis=2, concat_axis=0, tiled=True)
    update = whole_channels(gathered, out_weight, gate_value)
    return update.astype(jnp.bfloat16)


MESH = pl.DeviceIdType.MESH
LANES = 128
PIECES = 1
VMEM_BUDGET = 48 * 2**20


def up(value, step):
    return -(-value // step) * step


def fused_kernel(
    along_y, along_z,
    pair_ref, mask_ref, proj_ref, gate_ref, out_w_ref, out_ref,
    normed_bf, masked_bf, gate_f32, send_r, recv_r, recv_x, send_l, recv_l,
    left_s, right_s, tri_s, send_b, recv_b,
    ssem_r, rsem_r, ssem_x, rsem_x, ssem_l, rsem_l, ssem_b, rsem_b, own_sem,
):
    cols, rows, chans = pair_ref.shape
    hidden = out_w_ref.shape[0]
    groups = along_y * along_z
    gc = hidden // groups
    hc = gc // PIECES
    flat = rows * cols
    residues = mask_ref.shape[1]
    px, py, pz = lax.axis_index("gx"), lax.axis_index("gy"), lax.axis_index("gz")
    me = py * along_z + pz

    def place(d):
        return (px, d // along_z, d % along_z)

    partner = (1 - px, py, pz)
    barrier = pltpu.get_barrier_semaphore()

    def greet(o, carry):
        pl.semaphore_signal(barrier, inc=1, device_id=place((me + o) % groups), device_id_type=MESH)
        return carry

    lax.fori_loop(1, groups, greet, 0)
    pl.semaphore_signal(barrier, inc=1, device_id=partner, device_id_type=MESH)

    mask_f = mask_ref[...].astype(jnp.float32)
    lane = lax.broadcasted_iota(jnp.int32, (rows, residues), 1)
    sub = lax.broadcasted_iota(jnp.int32, (rows, residues), 0)
    row_mask = jnp.sum(jnp.where(lane == sub + px * rows, mask_f, 0.0), axis=1, keepdims=True)
    lane_row = lax.broadcasted_iota(jnp.int32, (1, residues), 1)
    for k in range(cols):
        col_mask = jnp.sum(
            jnp.where(lane_row == me * cols + k, mask_f, 0.0), axis=1, keepdims=True
        )
        normed = layer_norm_last(pair_ref[k].astype(jnp.float32)).astype(jnp.bfloat16)
        normed_bf[k * rows : (k + 1) * rows, :] = normed
        masked_bf[k * rows : (k + 1) * rows, :] = (
            normed.astype(jnp.float32) * (row_mask * col_mask)
        ).astype(jnp.bfloat16)

    proj_t = proj_ref[...].astype(jnp.float32).T.astype(jnp.bfloat16)
    masked = masked_bf[...]

    def project(first, count):
        return lax.dot_general(
            proj_t[first : first + count], masked, (((1,), (1,)), ((), ())),
            preferred_element_type=jnp.float32,
        )

    def copy_r(d, slot):
        return pltpu.make_async_remote_copy(
            src_ref=send_r.at[d], dst_ref=recv_r.at[slot], send_sem=ssem_r.at[d],
            recv_sem=rsem_r.at[slot], device_id=place(d), device_id_type=MESH,
        )

    def copy_l(h, d, slot):
        return pltpu.make_async_remote_copy(
            src_ref=send_l.at[h, d], dst_ref=recv_l.at[h, slot], send_sem=ssem_l.at[h, d],
            recv_sem=rsem_l.at[h, slot], device_id=place(d), device_id_type=MESH,
        )

    def copy_x(s):
        return pltpu.make_async_remote_copy(
            src_ref=recv_r.at[s], dst_ref=recv_x.at[s], send_sem=ssem_x.at[s],
            recv_sem=rsem_x.at[s], device_id=partner, device_id_type=MESH,
        )

    def copy_b(h, d, slot):
        return pltpu.make_async_remote_copy(
            src_ref=send_b.at[h, d], dst_ref=recv_b.at[h, slot], send_sem=ssem_b.at[h, d],
            recv_sem=rsem_b.at[h, slot], device_id=place(d), device_id_type=MESH,
        )

    step = 4 * gc

    def gated(first, side):
        base = 2 * side * hidden + first
        return jax.nn.sigmoid(project(base, step)) * project(base + hidden, step)

    for first in range(0, hidden, step):
        value = gated(first, 1)
        for part in range(step // gc):
            send_r[first // gc + part, :, 0:flat] = value[
                part * gc : (part + 1) * gc
            ].astype(jnp.bfloat16)

    pl.semaphore_wait(barrier, groups)

    def start_r(o, carry):
        copy_r((me + o) % groups, me).start()
        return carry

    lax.fori_loop(1, groups, start_r, 0)
    own_r = pltpu.make_async_copy(send_r.at[me], recv_r.at[me], own_sem.at[0])
    own_r.start()

    for first in range(0, hidden, step):
        value = gated(first, 0)
        for part in range(step // gc):
            for h in range(PIECES):
                low = part * gc + h * hc
                send_l[h, first // gc + part, :, 0:flat] = value[low : low + hc].astype(jnp.bfloat16)

    for h in range(PIECES):

        def start_l(o, carry, h=h):
            copy_l(h, (me + o) % groups, me).start()
            return carry

        lax.fori_loop(1, groups, start_l, 0)

    gate_f32[...] = jax.nn.sigmoid(
        jnp.dot(normed_bf[...], gate_ref[...], preferred_element_type=jnp.float32)
    )

    def spread(value, target, s, first, count):
        value = value.astype(jnp.float32)
        for k in range(cols):
            at = pl.multiple_of((s * cols + k) * gc, gc)
            target[pl.ds(at + first, count), 0:rows] = value[:, k * rows : (k + 1) * rows]

    own_r.wait()

    def take_r(o, carry):
        s = (me + groups - o) % groups

        @pl.when(o > 0)
        def _():
            copy_r(s, s).wait_recv()

        copy_x(s).start()
        spread(recv_r[s], right_s.at[px], s, 0, gc)
        return carry

    lax.fori_loop(0, groups, take_r, 0)

    def take_x(o, carry):
        s = (me + groups - o) % groups
        copy_x(s).wait_recv()
        spread(recv_x[s], right_s.at[1 - px], s, 0, gc)
        return carry

    lax.fori_loop(0, groups, take_x, 0)

    for h in range(PIECES):
        spread(send_l[h, me], left_s, me, h * hc, hc)

        def take_l(o, carry, h=h):
            s = (me + groups - o) % groups
            copy_l(h, s, s).wait_recv()
            spread(recv_l[h, s], left_s, s, h * hc, hc)
            return carry

        lax.fori_loop(1, groups, take_l, 0)

        for c in range(h * hc, (h + 1) * hc):
            left = left_s[pl.ds(c, residues, stride=gc), :].astype(jnp.bfloat16)
            for half in range(2):
                right = right_s[half, pl.ds(c, residues, stride=gc), :].astype(jnp.bfloat16)
                block = lax.dot_general(
                    right, left, (((0,), (0,)), ((), ())), preferred_element_type=jnp.float32
                )
                tri_s[pl.ds(half * rows * gc + c, rows, stride=gc), :] = block[0:rows]

        def pack_b(d, h=h):
            pieces = []
            for j in range(cols):
                at = pl.multiple_of((d * cols + j) * gc, gc)
                pieces.append(tri_s[pl.ds(at + h * hc, hc), 0:rows])
            return jnp.concatenate(pieces, axis=1).astype(jnp.bfloat16)

        def start_b(o, carry, h=h):
            d = (me + o) % groups
            send_b[h, d, :, 0:flat] = pack_b(d)
            copy_b(h, d, me).start()
            return carry

        lax.fori_loop(1, groups, start_b, 0)
        recv_b[h, me, :, 0:flat] = pack_b(me)

    for h in range(PIECES):

        def take_b(o, carry, h=h):
            s = (me + groups - o) % groups
            copy_b(h, s, s).wait_recv()
            return carry

        lax.fori_loop(1, groups, take_b, 0)

    triangle = jnp.concatenate(
        [recv_b[h, :, :, 0:flat].astype(jnp.float32) for h in range(PIECES)], axis=1
    ).reshape(hidden, flat)
    normed_tri = layer_norm_lead(triangle).astype(jnp.bfloat16)
    mixed = lax.dot_general(
        normed_tri, out_w_ref[...], (((0,), (0,)), ((), ())), preferred_element_type=jnp.float32
    )
    update = gate_f32[...] * mixed
    for j in range(cols):
        out_ref[j] = update[j * rows : (j + 1) * rows].astype(jnp.bfloat16)

    def finish(o, carry):
        d = (me + o) % groups
        copy_r(d, me).wait_send()
        for h in range(PIECES):
            copy_l(h, d, me).wait_send()
            copy_b(h, d, me).wait_send()
        return carry

    lax.fori_loop(1, groups, finish, 0)

    def finish_x(s, carry):
        copy_x(s).wait_send()
        return carry

    lax.fori_loop(0, groups, finish_x, 0)


def scratch_list(rows, cols, chans, hidden, groups, residues):
    gc = hidden // groups
    flat = up(rows * cols, LANES)
    hc = gc // PIECES
    bf, f32 = jnp.bfloat16, jnp.float32
    return [
        ((rows * cols, chans), bf),
        ((rows * cols, chans), bf),
        ((rows * cols, chans), f32),
        ((groups, gc, flat), bf),
        ((groups, gc, flat), bf),
        ((groups, gc, flat), bf),
        ((PIECES, groups, hc, flat), bf),
        ((PIECES, groups, hc, flat), bf),
        ((residues * gc, LANES), f32),
        ((2, residues * gc, LANES), f32),
        ((residues * gc, LANES), f32),
        ((PIECES, groups, hc, flat), bf),
        ((PIECES, groups, hc, flat), bf),
    ]


def fits_kernel(sizes, rows, cols, chans, hidden, residues):
    groups = sizes["gy"] * sizes["gz"]
    if sizes["gx"] != 2 or hidden % (4 * groups) or hidden // groups != 8:
        return False
    if chans != LANES or rows > LANES or rows % 16:
        return False
    total = 0
    for shape, kind in scratch_list(rows, cols, chans, hidden, groups, residues):
        count = 1
        for extent in shape:
            count *= extent
        total += count * jnp.dtype(kind).itemsize
    return total < VMEM_BUDGET // 4


def local_fused(sizes, pair_map, residue_mask, proj_weight, gate_weight, out_weight):
    rows, cols, chans = pair_map.shape
    hidden = out_weight.shape[0]
    residues = residue_mask.shape[0]
    if not fits_kernel(sizes, rows, cols, chans, hidden, residues):
        return local(pair_map, residue_mask, proj_weight, gate_weight, out_weight)
    groups = sizes["gy"] * sizes["gz"]
    dma = pltpu.SemaphoreType.DMA((groups,))
    dma_halves = pltpu.SemaphoreType.DMA((PIECES, groups))
    vmem = pl.BlockSpec(memory_space=pltpu.VMEM)
    turned = pl.pallas_call(
        functools.partial(fused_kernel, sizes["gy"], sizes["gz"]),
        out_shape=jax.ShapeDtypeStruct((cols, rows, chans), jnp.bfloat16),
        in_specs=[vmem] * 5,
        out_specs=vmem,
        scratch_shapes=[
            pltpu.VMEM(shape, kind)
            for shape, kind in scratch_list(rows, cols, chans, hidden, groups, residues)
        ]
        + [dma] * 4
        + [dma_halves] * 4
        + [pltpu.SemaphoreType.DMA((1,))],
        compiler_params=pltpu.CompilerParams(
            collective_id=0, has_side_effects=True, vmem_limit_bytes=VMEM_BUDGET
        ),
    )(
        pair_map.transpose(1, 0, 2), residue_mask.reshape(1, residues),
        proj_weight, gate_weight, out_weight,
    )
    return turned.transpose(1, 0, 2)


def solution(mesh):
    placed = (P("gx", ("gy", "gz"), None), P(), P(), P(), P())
    return jax.shard_map(
        functools.partial(local_fused, dict(mesh.shape)), mesh=mesh, in_specs=placed, out_specs=P("gx", ("gy", "gz"), None), check_vma=False
    )
```

```python
import functools

import jax
import jax.numpy as jnp
from jax import lax
from jax.experimental import pallas as pl
from jax.experimental.pallas import tpu as pltpu
from jax.sharding import PartitionSpec as P

epsilon = 1.0


def partner_2(x, axis, bit):
    return lax.ppermute(x, axis, [(i, i ^ 1 << bit) for i in range(lax.axis_size(axis))])


def layer_norm_lead(values):
    average = jnp.mean(values, axis=0, keepdims=True)
    centred = values - average
    variance = jnp.mean(centred * centred, axis=0, keepdims=True)
    return centred * lax.rsqrt(variance + epsilon)


def layer_norm_last(values):
    average = jnp.mean(values, axis=-1, keepdims=True)
    centred = values - average
    variance = jnp.mean(centred * centred, axis=-1, keepdims=True)
    return centred * lax.rsqrt(variance + epsilon)


def swap_with(values, bit):
    return partner_2(values, "gx", bit)


def pair_join(values, bit, position):
    partner = swap_with(values, bit)
    mine_first = position // 2**bit % 2 == 0
    return jnp.where(
        mine_first,
        jnp.concatenate([values, partner], axis=1),
        jnp.concatenate([partner, values], axis=1),
    )


def whole_channels(gathered, out_weight, gate_value):
    hidden, row_count, col_count = gathered.shape
    normed_tri = layer_norm_lead(gathered.astype(jnp.float32)).astype(jnp.bfloat16)
    mixed_out = lax.dot_general(
        normed_tri.reshape(hidden, row_count * col_count),
        out_weight,
        (((0,), (0,)), ((), ())),
        preferred_element_type=jnp.float32,
    )
    return gate_value * mixed_out.reshape(row_count, col_count, out_weight.shape[1])


def local(pair_map, residue_mask, proj_weight, gate_weight, out_weight):
    row_count, col_count, chan_count = pair_map.shape
    hidden = out_weight.shape[0]
    residues = residue_mask.shape[0]
    along_x = lax.axis_size("gx")
    along_y = lax.axis_size("gy")
    along_z = lax.axis_size("gz")
    mask_float = residue_mask.astype(jnp.float32)
    row_mask = lax.dynamic_slice_in_dim(mask_float, lax.axis_index("gx") * row_count, row_count)
    col_mask = lax.dynamic_slice_in_dim(
        mask_float, (lax.axis_index("gy") * along_z + lax.axis_index("gz")) * col_count, col_count
    )
    normed = layer_norm_last(pair_map.astype(jnp.float32)).astype(jnp.bfloat16)
    flattened = normed.reshape(row_count * col_count, chan_count)
    projected = lax.dot_general(
        proj_weight, flattened, (((0,), (1,)), ((), ())), preferred_element_type=jnp.float32
    ).reshape(4 * hidden, row_count, col_count)
    pair_mask = (row_mask[:, None] * col_mask[None, :])[None, :, :]
    left_proj = (
        jax.nn.sigmoid(projected[:hidden]) * projected[hidden : 2 * hidden] * pair_mask
    ).astype(jnp.bfloat16)
    right_proj = (
        jax.nn.sigmoid(projected[2 * hidden : 3 * hidden]) * projected[3 * hidden :] * pair_mask
    ).astype(jnp.bfloat16)
    gate_value = jax.nn.sigmoid(
        jnp.dot(flattened, gate_weight, preferred_element_type=jnp.float32)
    ).reshape(row_count, col_count, chan_count)
    group_count = along_y * along_z
    group_chan = hidden // group_count
    left_group, right_group = (
        lax.all_to_all(left_proj, ("gy", "gz"), split_axis=0, concat_axis=2, tiled=True),
        lax.all_to_all(right_proj, ("gy", "gz"), split_axis=0, concat_axis=2, tiled=True),
    )
    levels = along_x.bit_length() - 1
    low_bits = levels // 2
    high_count = 2 ** (levels - low_bits)
    low_count = 2**low_bits
    position = lax.axis_index("gx")
    left_tile = left_group
    for bit in range(low_bits):
        left_tile = pair_join(left_tile, bit, position)
    right_tile = right_group
    for bit in range(low_bits, levels):
        right_tile = pair_join(right_tile, bit, position)
    block_tile = jnp.einsum(
        "cik,cjk->cij", left_tile, right_tile, preferred_element_type=jnp.float32
    ).astype(jnp.bfloat16)
    for bit in range(low_bits):
        current = block_tile.shape[1]
        span = block_tile.shape[2]
        shaped = block_tile.reshape(group_chan, current // (2 * row_count), 2, row_count, span)
        own_bit = position // 2**bit % 2
        kept = lax.dynamic_index_in_dim(shaped, own_bit, axis=2, keepdims=False).reshape(
            group_chan, current // 2, span
        )
        sent = lax.dynamic_index_in_dim(shaped, 1 - own_bit, axis=2, keepdims=False).reshape(
            group_chan, current // 2, span
        )
        arrived = swap_with(sent, bit)
        block_tile = jnp.where(
            own_bit == 0,
            jnp.concatenate([kept, arrived], axis=2),
            jnp.concatenate([arrived, kept], axis=2),
        )
    block_tile = (
        block_tile.reshape(group_chan, row_count, low_count, high_count, row_count)
        .transpose(0, 1, 3, 2, 4)
        .reshape(group_chan, row_count, residues)
    )
    gathered = lax.all_to_all(block_tile, ("gy", "gz"), split_axis=2, concat_axis=0, tiled=True)
    update = whole_channels(gathered, out_weight, gate_value)
    return update.astype(jnp.bfloat16)


MESH = pl.DeviceIdType.MESH
LANES = 128
PIECES = 1
VMEM_GRANT = 67043328
VMEM_BUDGET = 48 * 2**20


def up(value, step):
    return -(-value // step) * step


def fused_kernel(
    along_y, along_z,
    pair_hbm, mask_hbm, proj_hbm, gate_hbm, out_w_hbm, out_ref,
    pair_ref, mask_ref, proj_ref, gate_ref, out_w_ref,
    normed_bf, masked_bf, gate_f32, send_r, recv_r, recv_x, send_l, recv_l,
    left_s, right_s, tri_s, send_b, recv_b,
    ssem_r, rsem_r, ssem_x, rsem_x, ssem_l, rsem_l, ssem_b, rsem_b, own_sem, load_sem,
):
    cols, rows, chans = pair_ref.shape
    hidden = out_w_ref.shape[0]
    groups = along_y * along_z
    gc = hidden // groups
    hc = gc // PIECES
    flat = rows * cols
    residues = mask_ref.shape[1]
    px, py, pz = lax.axis_index("gx"), lax.axis_index("gy"), lax.axis_index("gz")
    me = py * along_z + pz

    def place(d):
        return (px, d // along_z, d % along_z)

    partner = (1 - px, py, pz)
    barrier = pltpu.get_barrier_semaphore()

    def greet(o, carry):
        pl.semaphore_signal(barrier, inc=1, device_id=place((me + o) % groups), device_id_type=MESH)
        return carry

    lax.fori_loop(1, groups, greet, 0)
    pl.semaphore_signal(barrier, inc=1, device_id=partner, device_id_type=MESH)

    loads = [
        pltpu.make_async_copy(source, target, load_sem.at[n])
        for n, (source, target) in enumerate(
            (
                (pair_hbm, pair_ref), (mask_hbm, mask_ref), (proj_hbm, proj_ref),
                (gate_hbm, gate_ref), (out_w_hbm, out_w_ref),
            )
        )
    ]
    for load in loads:
        load.start()
    loads[0].wait()
    loads[1].wait()

    mask_f = mask_ref[...].astype(jnp.float32)
    lane = lax.broadcasted_iota(jnp.int32, (rows, residues), 1)
    sub = lax.broadcasted_iota(jnp.int32, (rows, residues), 0)
    row_mask = jnp.sum(jnp.where(lane == sub + px * rows, mask_f, 0.0), axis=1, keepdims=True)
    lane_row = lax.broadcasted_iota(jnp.int32, (1, residues), 1)
    for k in range(cols):
        col_mask = jnp.sum(
            jnp.where(lane_row == me * cols + k, mask_f, 0.0), axis=1, keepdims=True
        )
        normed = layer_norm_last(pair_ref[k].astype(jnp.float32)).astype(jnp.bfloat16)
        normed_bf[k * rows : (k + 1) * rows, :] = normed
        masked_bf[k * rows : (k + 1) * rows, :] = (
            normed.astype(jnp.float32) * (row_mask * col_mask)
        ).astype(jnp.bfloat16)

    loads[2].wait()
    proj_t = proj_ref[...].astype(jnp.float32).T.astype(jnp.bfloat16)
    masked = masked_bf[...]

    def project(first, count):
        return lax.dot_general(
            proj_t[first : first + count], masked, (((1,), (1,)), ((), ())),
            preferred_element_type=jnp.float32,
        )

    def copy_r(d, slot):
        return pltpu.make_async_remote_copy(
            src_ref=send_r.at[d], dst_ref=recv_r.at[slot], send_sem=ssem_r.at[d],
            recv_sem=rsem_r.at[slot], device_id=place(d), device_id_type=MESH,
        )

    def copy_l(h, d, slot):
        return pltpu.make_async_remote_copy(
            src_ref=send_l.at[h, d], dst_ref=recv_l.at[h, slot], send_sem=ssem_l.at[h, d],
            recv_sem=rsem_l.at[h, slot], device_id=place(d), device_id_type=MESH,
        )

    def copy_x(s):
        return pltpu.make_async_remote_copy(
            src_ref=recv_r.at[s], dst_ref=recv_x.at[s], send_sem=ssem_x.at[s],
            recv_sem=rsem_x.at[s], device_id=partner, device_id_type=MESH,
        )

    def copy_b(h, d, slot):
        return pltpu.make_async_remote_copy(
            src_ref=send_b.at[h, d], dst_ref=recv_b.at[h, slot], send_sem=ssem_b.at[h, d],
            recv_sem=rsem_b.at[h, slot], device_id=place(d), device_id_type=MESH,
        )

    step = 4 * gc

    def gated(first, side):
        base = 2 * side * hidden + first
        return jax.nn.sigmoid(project(base, step)) * project(base + hidden, step)

    for first in range(0, hidden, step):
        value = gated(first, 1)
        for part in range(step // gc):
            send_r[first // gc + part, :, 0:flat] = value[
                part * gc : (part + 1) * gc
            ].astype(jnp.bfloat16)

    pl.semaphore_wait(barrier, groups)

    def start_r(o, carry):
        copy_r((me + o) % groups, me).start()
        return carry

    lax.fori_loop(1, groups, start_r, 0)
    own_r = pltpu.make_async_copy(send_r.at[me], recv_r.at[me], own_sem.at[0])
    own_r.start()

    for first in range(0, hidden, step):
        value = gated(first, 0)
        for part in range(step // gc):
            for h in range(PIECES):
                low = part * gc + h * hc
                send_l[h, first // gc + part, :, 0:flat] = value[low : low + hc].astype(jnp.bfloat16)

    for h in range(PIECES):

        def start_l(o, carry, h=h):
            copy_l(h, (me + o) % groups, me).start()
            return carry

        lax.fori_loop(1, groups, start_l, 0)

    loads[3].wait()
    loads[4].wait()
    gate_f32[...] = jax.nn.sigmoid(
        jnp.dot(normed_bf[...], gate_ref[...], preferred_element_type=jnp.float32)
    )

    def spread(value, target, s, first, count):
        value = value.astype(jnp.float32)
        for k in range(cols):
            at = pl.multiple_of((s * cols + k) * gc, gc)
            target[pl.ds(at + first, count), 0:rows] = value[:, k * rows : (k + 1) * rows]

    own_r.wait()

    def take_r(o, carry):
        s = (me + groups - o) % groups

        @pl.when(o > 0)
        def _():
            copy_r(s, s).wait_recv()

        copy_x(s).start()
        spread(recv_r[s], right_s.at[px], s, 0, gc)
        return carry

    lax.fori_loop(0, groups, take_r, 0)

    def take_x(o, carry):
        s = (me + groups - o) % groups
        copy_x(s).wait_recv()
        spread(recv_x[s], right_s.at[1 - px], s, 0, gc)
        return carry

    lax.fori_loop(0, groups, take_x, 0)

    for h in range(PIECES):
        spread(send_l[h, me], left_s, me, h * hc, hc)

        def take_l(o, carry, h=h):
            s = (me + groups - o) % groups
            copy_l(h, s, s).wait_recv()
            spread(recv_l[h, s], left_s, s, h * hc, hc)
            return carry

        lax.fori_loop(1, groups, take_l, 0)

        for c in range(h * hc, (h + 1) * hc):
            left = left_s[pl.ds(c, residues, stride=gc), :].astype(jnp.bfloat16)
            for half in range(2):
                right = right_s[half, pl.ds(c, residues, stride=gc), :].astype(jnp.bfloat16)
                block = lax.dot_general(
                    right, left, (((0,), (0,)), ((), ())), preferred_element_type=jnp.float32
                )
                tri_s[pl.ds(half * rows * gc + c, rows, stride=gc), :] = block[0:rows]

        def pack_b(d, h=h):
            pieces = []
            for j in range(cols):
                at = pl.multiple_of((d * cols + j) * gc, gc)
                pieces.append(tri_s[pl.ds(at + h * hc, hc), 0:rows])
            return jnp.concatenate(pieces, axis=1).astype(jnp.bfloat16)

        def start_b(o, carry, h=h):
            d = (me + o) % groups
            send_b[h, d, :, 0:flat] = pack_b(d)
            copy_b(h, d, me).start()
            return carry

        lax.fori_loop(1, groups, start_b, 0)
        recv_b[h, me, :, 0:flat] = pack_b(me)

    for h in range(PIECES):

        def take_b(o, carry, h=h):
            s = (me + groups - o) % groups
            copy_b(h, s, s).wait_recv()
            return carry

        lax.fori_loop(1, groups, take_b, 0)

    triangle = jnp.concatenate(
        [recv_b[h, :, :, 0:flat].astype(jnp.float32) for h in range(PIECES)], axis=1
    ).reshape(hidden, flat)
    normed_tri = layer_norm_lead(triangle).astype(jnp.bfloat16)
    mixed = lax.dot_general(
        normed_tri, out_w_ref[...], (((0,), (0,)), ((), ())), preferred_element_type=jnp.float32
    )
    update = gate_f32[...] * mixed
    for j in range(cols):
        out_ref[j] = update[j * rows : (j + 1) * rows].astype(jnp.bfloat16)

    def finish(o, carry):
        d = (me + o) % groups
        copy_r(d, me).wait_send()
        for h in range(PIECES):
            copy_l(h, d, me).wait_send()
            copy_b(h, d, me).wait_send()
        return carry

    lax.fori_loop(1, groups, finish, 0)

    def finish_x(s, carry):
        copy_x(s).wait_send()
        return carry

    lax.fori_loop(0, groups, finish_x, 0)


def scratch_list(rows, cols, chans, hidden, groups, residues):
    gc = hidden // groups
    flat = up(rows * cols, LANES)
    hc = gc // PIECES
    bf, f32 = jnp.bfloat16, jnp.float32
    return [
        ((cols, rows, chans), bf),
        ((1, residues), jnp.int32),
        ((chans, 4 * hidden), bf),
        ((chans, chans), bf),
        ((hidden, chans), bf),
        ((rows * cols, chans), bf),
        ((rows * cols, chans), bf),
        ((rows * cols, chans), f32),
        ((groups, gc, flat), bf),
        ((groups, gc, flat), bf),
        ((groups, gc, flat), bf),
        ((PIECES, groups, hc, flat), bf),
        ((PIECES, groups, hc, flat), bf),
        ((residues * gc, LANES), f32),
        ((2, residues * gc, LANES), f32),
        ((residues * gc, LANES), f32),
        ((PIECES, groups, hc, flat), bf),
        ((PIECES, groups, hc, flat), bf),
    ]


def fits_kernel(sizes, rows, cols, chans, hidden, residues):
    groups = sizes["gy"] * sizes["gz"]
    if sizes["gx"] != 2 or hidden % (4 * groups) or hidden // groups != 8:
        return False
    if chans != LANES or rows > LANES or rows % 16:
        return False
    total = 0
    for shape, kind in scratch_list(rows, cols, chans, hidden, groups, residues):
        count = 1
        for extent in shape:
            count *= extent
        total += count * jnp.dtype(kind).itemsize
    return total < VMEM_BUDGET // 4


def local_fused(sizes, pair_map, residue_mask, proj_weight, gate_weight, out_weight):
    rows, cols, chans = pair_map.shape
    hidden = out_weight.shape[0]
    residues = residue_mask.shape[0]
    if not fits_kernel(sizes, rows, cols, chans, hidden, residues):
        return local(pair_map, residue_mask, proj_weight, gate_weight, out_weight)
    groups = sizes["gy"] * sizes["gz"]
    dma = pltpu.SemaphoreType.DMA((groups,))
    dma_halves = pltpu.SemaphoreType.DMA((PIECES, groups))
    vmem = pl.BlockSpec(memory_space=pltpu.VMEM)
    turned = pl.pallas_call(
        functools.partial(fused_kernel, sizes["gy"], sizes["gz"]),
        out_shape=jax.ShapeDtypeStruct((cols, rows, chans), jnp.bfloat16),
        in_specs=[pl.BlockSpec(memory_space=pltpu.HBM)] * 5,
        out_specs=vmem,
        scratch_shapes=[
            pltpu.VMEM(shape, kind)
            for shape, kind in scratch_list(rows, cols, chans, hidden, groups, residues)
        ]
        + [dma] * 4
        + [dma_halves] * 4
        + [pltpu.SemaphoreType.DMA((1,)), pltpu.SemaphoreType.DMA((5,))],
        compiler_params=pltpu.CompilerParams(
            collective_id=0, has_side_effects=True, vmem_limit_bytes=VMEM_GRANT
        ),
    )(
        pair_map.transpose(1, 0, 2), residue_mask.reshape(1, residues),
        proj_weight, gate_weight, out_weight,
    )
    return turned.transpose(1, 0, 2)


def solution(mesh):
    placed = (P("gx", ("gy", "gz"), None), P(), P(), P(), P())
    return jax.shard_map(
        functools.partial(local_fused, dict(mesh.shape)), mesh=mesh, in_specs=placed, out_specs=P("gx", ("gy", "gz"), None), check_vma=False
    )
```
